8 devices in a mesh: tp: 4 (over z, y, x), dp: 2 (over core).
Axes of the slice: x: 2, y: 2, z: 1, core: 2. Of those that a mesh axis runs over, the one named last changes fastest.
Arguments:
- x: bfloat16 [8, 2048, 1536], P('dp')
- lengths: int32 [8], P('dp')
- targets: int32 [8], P('dp')
- norm1: bfloat16 [2, 1536], replicated
- norm2: bfloat16 [2, 1536], replicated
- norm_f: bfloat16 [1536], replicated
- w_q: bfloat16 [2, 1536, 12, 128], P(None, ('dp', 'tp'))
- w_k: bfloat16 [2, 1536, 2, 128], P(None, ('dp', 'tp'))
- w_v: bfloat16 [2, 1536, 2, 128], P(None, ('dp', 'tp'))
- w_o: bfloat16 [2, 1536, 1536], P(None, ('dp', 'tp'))
- w_gate: bfloat16 [2, 1536, 8960], P(None, ('dp', 'tp'))
- w_up: bfloat16 [2, 1536, 8960], P(None, ('dp', 'tp'))
- w_down: bfloat16 [2, 8960, 1536], P(None, ('dp', 'tp'))
- w_lm: bfloat16 [1536, 151936], P(('dp', 'tp'))
Outputs:
- output 1: bfloat16 [2, 1536, 12, 128], P(None, None, 'tp')
- output 2: bfloat16 [2, 1536, 4, 128], P(None, None, 'tp')
- output 3: bfloat16 [2, 1536, 4, 128], P(None, None, 'tp')
- output 4: bfloat16 [2, 1536, 1536], P(None, 'tp')
- output 5: bfloat16 [2, 1536, 8960], P(None, None, 'tp')
- output 6: bfloat16 [2, 1536, 8960], P(None, None, 'tp')
- output 7: bfloat16 [2, 8960, 1536], P(None, 'tp')
- output 8: bfloat16 [2, 8, 4, 2048, 128], P(None, 'dp', 'tp')
- output 9: bfloat16 [2, 8, 4, 2048, 128], P(None, 'dp', 'tp')
- output 10: float32 [8], P('dp')
All inputs are finite; a program needn't handle non-finite values.
Results may differ from the reference program's by a relative error of at most 0.0107616.
Values are sent between devices in bfloat16 or wider.
A program may use at most 1 GiB of HBM per device.

```python
import jax
import jax.numpy as jnp
from jax import lax

MODEL_DIM = 1536
Q_HEADS = 12
KV_HEADS = 2
HEAD_DIM = 128
FFN_DIM = 8960
VOCAB_SIZE = 151936
SEQ_LEN = 2048
NUM_LAYERS = 2
TP_SIZE = 4
BATCH_ALL = 8

ROPE_BASE = 10000.0
NORM_EPS = 1e-6


def draw_normal(rng_key, shape, scale):
    return (jax.random.normal(rng_key, shape, jnp.float32) * scale).astype(jnp.bfloat16)


def draw_gain(rng_key, shape):
    return jax.random.uniform(rng_key, shape, jnp.float32, 0.5, 1.5).astype(jnp.bfloat16)


def setup_inputs(seed: int = 0) -> dict:
    subkeys = jax.random.split(jax.random.key(seed), 16)
    q_width = Q_HEADS * HEAD_DIM
    lengths = jax.random.randint(subkeys[0], (BATCH_ALL,), SEQ_LEN // 4, SEQ_LEN + 1, jnp.int32)
    full_at = jax.random.randint(subkeys[1], (), 0, BATCH_ALL, jnp.int32)
    lengths = jnp.where(jnp.arange(BATCH_ALL) == full_at, SEQ_LEN, lengths).astype(jnp.int32)
    targets = jax.random.randint(subkeys[2], (BATCH_ALL,), 0, VOCAB_SIZE, jnp.int32)
    dim_scale = MODEL_DIM ** -0.5
    return dict(
        x=draw_normal(subkeys[3], (BATCH_ALL, SEQ_LEN, MODEL_DIM), 1.0),
        lengths=lengths,
        targets=targets,
        norm1=draw_gain(subkeys[4], (NUM_LAYERS, MODEL_DIM)),
        norm2=draw_gain(subkeys[5], (NUM_LAYERS, MODEL_DIM)),
        norm_f=draw_gain(subkeys[6], (MODEL_DIM,)),
        w_q=draw_normal(subkeys[7], (NUM_LAYERS, MODEL_DIM, Q_HEADS, HEAD_DIM), 2.0 * dim_scale),
        w_k=draw_normal(subkeys[8], (NUM_LAYERS, MODEL_DIM, KV_HEADS, HEAD_DIM), dim_scale),
        w_v=draw_normal(subkeys[9], (NUM_LAYERS, MODEL_DIM, KV_HEADS, HEAD_DIM), dim_scale),
        w_o=draw_normal(subkeys[10], (NUM_LAYERS, q_width, MODEL_DIM), 2.0 * q_width ** -0.5),
        w_gate=draw_normal(subkeys[11], (NUM_LAYERS, MODEL_DIM, FFN_DIM), dim_scale),
        w_up=draw_normal(subkeys[12], (NUM_LAYERS, MODEL_DIM, FFN_DIM), dim_scale),
        w_down=draw_normal(subkeys[13], (NUM_LAYERS, FFN_DIM, MODEL_DIM), FFN_DIM ** -0.5),
        w_lm=draw_normal(subkeys[14], (MODEL_DIM, VOCAB_SIZE), 2.0 * dim_scale),
    )


def rms_scale(hidden, gain):
    hidden32 = hidden.astype(jnp.float32)
    inv_rms = lax.rsqrt(jnp.mean(hidden32 * hidden32, axis=-1, keepdims=True) + NORM_EPS)
    return (hidden32 * inv_rms * gain.astype(jnp.float32)).astype(jnp.bfloat16)


def rope_tables():
    positions = jnp.arange(SEQ_LEN, dtype=jnp.float32)
    inv_freq = ROPE_BASE ** (-2.0 * jnp.arange(HEAD_DIM // 2, dtype=jnp.float32) / HEAD_DIM)
    angles = positions[:, None] * inv_freq[None, :]
    return jnp.cos(angles), jnp.sin(angles)


def apply_rope(projected, cos_tab, sin_tab):
    half_dim = projected.shape[-1] // 2
    lower_half = projected[..., :half_dim]
    upper_half = projected[..., half_dim:]
    cos_rows = cos_tab[:, None, :]
    sin_rows = sin_tab[:, None, :]
    return jnp.concatenate([lower_half * cos_rows - upper_half * sin_rows, upper_half * cos_rows + lower_half * sin_rows], axis=-1)


def residual_add(hidden, update):
    return (hidden.astype(jnp.float32) + update.astype(jnp.float32)).astype(jnp.bfloat16)


def reference(x, lengths, targets, norm1, norm2, norm_f, w_q, w_k, w_v, w_o, w_gate, w_up, w_down, w_lm):
    cos_tab, sin_tab = rope_tables()
    positions = jnp.arange(SEQ_LEN)
    group_size = Q_HEADS // KV_HEADS
    replicas = TP_SIZE // KV_HEADS
    score_scale = HEAD_DIM ** -0.5
    layer_weights = (norm1, norm2, w_q, w_k, w_v, w_o, w_gate, w_up, w_down)

    def one_sequence(seq_args):
        hidden, length, target = seq_args
        visible = (positions[None, :] <= positions[:, None]) & (positions[None, :] < length)

        def layer_step(resid, weights):
            gain_attn, gain_mlp, wq_l, wk_l, wv_l, wo_l, wg_l, wu_l, wd_l = weights
            normed = rms_scale(resid, gain_attn)
            q_proj = jnp.dot(normed, wq_l.reshape(MODEL_DIM, Q_HEADS * HEAD_DIM), preferred_element_type=jnp.float32)
            q_rot = apply_rope(q_proj.reshape(SEQ_LEN, Q_HEADS, HEAD_DIM), cos_tab, sin_tab).astype(jnp.bfloat16)
            k_proj = jnp.dot(normed, wk_l.reshape(MODEL_DIM, KV_HEADS * HEAD_DIM), preferred_element_type=jnp.float32)
            k_rot = apply_rope(k_proj.reshape(SEQ_LEN, KV_HEADS, HEAD_DIM), cos_tab, sin_tab).astype(jnp.bfloat16)
            v_proj = jnp.dot(normed, wv_l.reshape(MODEL_DIM, KV_HEADS * HEAD_DIM), preferred_element_type=jnp.float32)
            v_proj = v_proj.astype(jnp.bfloat16).reshape(SEQ_LEN, KV_HEADS, HEAD_DIM)
            q_grp = q_rot.reshape(SEQ_LEN, KV_HEADS, group_size, HEAD_DIM).astype(jnp.float32)
            scores = jnp.einsum('skgd,tkd->kgst', q_grp, k_rot.astype(jnp.float32)) * score_scale
            scores = jnp.where(visible, scores, -1e30)
            attn_probs = jax.nn.softmax(scores, axis=-1).astype(jnp.bfloat16)
            attn_mix = jnp.einsum('kgst,tkd->skgd', attn_probs.astype(jnp.float32), v_proj.astype(jnp.float32)).astype(jnp.bfloat16)
            attn_out = jnp.dot(attn_mix.reshape(SEQ_LEN, Q_HEADS * HEAD_DIM), wo_l, preferred_element_type=jnp.float32).astype(jnp.bfloat16)
            resid = residual_add(resid, attn_out)
            normed2 = rms_scale(resid, gain_mlp)
            gate_proj = jnp.dot(normed2, wg_l, preferred_element_type=jnp.float32)
            up_proj = jnp.dot(normed2, wu_l, preferred_element_type=jnp.float32)
            activated = (jax.nn.silu(gate_proj) * up_proj).astype(jnp.bfloat16)
            down_out = jnp.dot(activated, wd_l, preferred_element_type=jnp.float32).astype(jnp.bfloat16)
            resid = residual_add(resid, down_out)
            return resid, (jnp.swapaxes(k_rot, 0, 1), jnp.swapaxes(v_proj, 0, 1))

        final, (k_layers, v_layers) = lax.scan(layer_step, hidden, layer_weights)
        last_row = lax.dynamic_slice_in_dim(final, length - 1, 1, axis=0)
        logits = jnp.dot(rms_scale(last_row, norm_f), w_lm, preferred_element_type=jnp.float32)[0]
        logprob = lax.dynamic_index_in_dim(logits, target, keepdims=False) - jax.nn.logsumexp(logits)
        return k_layers, v_layers, logprob

    k_all, v_all, logprob = lax.map(one_sequence, (x, lengths, targets))
    k_cache = jnp.repeat(jnp.swapaxes(k_all, 0, 1), replicas, axis=2)
    v_cache = jnp.repeat(jnp.swapaxes(v_all, 0, 1), replicas, axis=2)
    k_out = jnp.repeat(w_k, replicas, axis=2)
    v_out = jnp.repeat(w_v, replicas, axis=2)
    return (w_q, k_out, v_out, w_o, w_gate, w_up, w_down, k_cache, v_cache, logprob)
```

```python
import functools
import math

import jax
import jax.numpy as jnp
from jax import lax
from jax.experimental import pallas as pl
from jax.experimental.pallas import tpu as pltpu
from jax.sharding import PartitionSpec as P


ROPE_BASE = 10000.0
NORM_EPS = 1e-6
F32 = jnp.float32
BF16 = jnp.bfloat16


def rms_scale(hidden, gain):
    hidden32 = hidden.astype(F32)
    inv_rms = lax.rsqrt(jnp.mean(hidden32 * hidden32, axis=-1, keepdims=True) + NORM_EPS)
    return (hidden32 * inv_rms * gain.astype(F32)).astype(BF16)


def rope_tables(positions, head_dim):
    inv_freq = ROPE_BASE ** (-2.0 * jnp.arange(head_dim // 2, dtype=F32) / head_dim)
    angles = positions.astype(F32)[:, None] * inv_freq[None, :]
    return jnp.cos(angles), jnp.sin(angles)


def residual_add(hidden, update):
    return (hidden.astype(F32) + update.astype(F32)).astype(BF16)


def dot32(a, b):
    return jnp.dot(a, b, preferred_element_type=F32)


def roped_kernel(n_rope, head_dim, idx_ref, x_ref, gain_ref, w_ref, cos_ref, sin_ref, o_ref):
    x32 = x_ref[0].astype(F32)
    inv_rms = lax.rsqrt(jnp.mean(x32 * x32, axis=-1, keepdims=True) + NORM_EPS)
    z = (x32 * inv_rms * gain_ref[...]).astype(BF16)
    width = w_ref.shape[1]
    chunk = 2 * head_dim if width % (2 * head_dim) == 0 else head_dim
    for start in range(0, width, chunk):
        p = dot32(z, w_ref[:, start:start + chunk])
        for off in range(0, chunk, head_dim):
            piece = p[:, off:off + head_dim]
            if (start + off) // head_dim < n_rope:
                piece = piece * cos_ref[...] + pltpu.roll(piece, head_dim // 2, 1) * sin_ref[...]
            o_ref[:, start + off:start + off + head_dim] = piece.astype(BF16)


def norm_proj_rope(x, which, n_seq, gain, w, col_block, width, n_rope, cos_full, sin_full):
    _, seq_len, model_dim = x.shape
    head_dim = cos_full.shape[1]
    bm = 256
    per = seq_len // bm
    return pl.pallas_call(
        functools.partial(roped_kernel, n_rope, head_dim),
        grid_spec=pltpu.PrefetchScalarGridSpec(
            num_scalar_prefetch=1,
            grid=(n_seq * per,),
            in_specs=[
                pl.BlockSpec((1, bm, model_dim), lambda i, s: (s[0] + i // per, i % per, 0)),
                pl.BlockSpec((1, model_dim), lambda i, s: (0, 0)),
                pl.BlockSpec((model_dim, width), lambda i, s: (0, col_block)),
                pl.BlockSpec((bm, head_dim), lambda i, s: (i % per, 0)),
                pl.BlockSpec((bm, head_dim), lambda i, s: (i % per, 0)),
            ],
            out_specs=pl.BlockSpec((bm, width), lambda i, s: (i, 0)),
        ),
        out_shape=jax.ShapeDtypeStruct((n_seq * seq_len, width), BF16),
        compiler_params=pltpu.CompilerParams(dimension_semantics=("arbitrary",)),
        cost_estimate=pl.CostEstimate(flops=2 * n_seq * seq_len * model_dim * width, bytes_accessed=2 * n_seq * seq_len * (model_dim + width), transcendentals=0),
        name="norm_proj_rope",
    )(which, x, gain.astype(F32)[None], w, cos_full, sin_full)


def out_proj_kernel(idx_ref, mix_ref, w_ref, x_ref, gain_ref, h_ref, z_ref):
    update = dot32(mix_ref[...], w_ref[...]).astype(BF16)
    hidden = residual_add(x_ref[0], update)
    h_ref[...] = hidden
    z_ref[...] = rms_scale(hidden, gain_ref[...])


def out_proj_norm(x, which, mix, w, gain):
    _, seq_len, model_dim = x.shape
    bm = 256
    row = jax.ShapeDtypeStruct((seq_len, model_dim), BF16)
    return pl.pallas_call(
        out_proj_kernel,
        grid_spec=pltpu.PrefetchScalarGridSpec(
            num_scalar_prefetch=1,
            grid=(seq_len // bm,),
            in_specs=[
                pl.BlockSpec((bm, mix.shape[1]), lambda i, s: (i, 0)),
                pl.BlockSpec(w.shape, lambda i, s: (0, 0)),
                pl.BlockSpec((1, bm, model_dim), lambda i, s: (s[0], i, 0)),
                pl.BlockSpec((1, model_dim), lambda i, s: (0, 0)),
            ],
            out_specs=[pl.BlockSpec((bm, model_dim), lambda i, s: (i, 0))] * 2,
        ),
        out_shape=[row, row],
        compiler_params=pltpu.CompilerParams(dimension_semantics=("arbitrary",)),
        cost_estimate=pl.CostEstimate(flops=2 * seq_len * model_dim * model_dim, bytes_accessed=8 * seq_len * model_dim, transcendentals=0),
        name="out_proj_norm",
    )(which, mix, w, x, gain.astype(F32)[None])


def block_t_kernel(win, cols, bm, off_ref, w_ref, *rest):
    o_ref, buf, sem = rest[-3:]
    i = pl.program_id(0)

    def fetch(j):
        src = w_ref.at[pl.ds(j * bm, bm), pl.ds(pl.multiple_of(off_ref[0], 128), win)]
        return pltpu.make_async_copy(src, buf.at[j % 2], sem.at[j % 2])

    @pl.when(i == 0)
    def _():
        fetch(i).start()

    @pl.when(i + 1 < pl.num_programs(0))
    def _():
        fetch(i + 1).start()

    fetch(i).wait()
    flipped = buf[i % 2].T
    o_ref[0] = jnp.where(off_ref[1] == 1, flipped[win - cols:, :], flipped[:cols, :])


def block_transposed(w, layer, n_layers, off, cols, prev):
    rows = w.shape[0]
    bm, win = 128, (cols + 127) // 128 * 128
    off = jnp.stack([off // 128 * 128, jnp.where(off % 128 != 0, 1, 0)]).astype(jnp.int32)
    extra = () if prev is None else (prev,)
    return pl.pallas_call(
        functools.partial(block_t_kernel, win, cols, bm),
        grid_spec=pltpu.PrefetchScalarGridSpec(
            num_scalar_prefetch=1,
            grid=(rows // bm,),
            in_specs=[pl.BlockSpec(memory_space=pl.ANY)] * (1 + len(extra)),
            out_specs=pl.BlockSpec((1, cols, bm), lambda i, s: (layer, 0, i)),
            scratch_shapes=[pltpu.VMEM((2, bm, win), BF16), pltpu.SemaphoreType.DMA((2,))],
        ),
        out_shape=jax.ShapeDtypeStruct((n_layers, cols, rows), BF16),
        input_output_aliases={} if prev is None else {2: 0},
        compiler_params=pltpu.CompilerParams(dimension_semantics=("arbitrary",)),
        cost_estimate=pl.CostEstimate(flops=20 * rows * win * 128, bytes_accessed=4 * rows * cols, transcendentals=0),
        name="block_transposed",
    )(off, w, *extra)


def pieces_t_kernel(col, win, cols, rows, n_pieces, idx_ref, *refs):
    pieces, (o_ref, buf, sem) = refs[:n_pieces], refs[-3:]
    i = pl.program_id(0)

    def fetch(j, run):
        for k, ref in enumerate(pieces):
            @pl.when(j == k // 2)
            def _():
                half = (k % 2) ^ idx_ref[0]
                copy = pltpu.make_async_copy(ref.at[:, pl.ds(col, win)], buf.at[j % 2, pl.ds(half * rows, rows)], sem.at[j % 2, k % 2])
                copy.start() if run else copy.wait()

    @pl.when(i == 0)
    def _():
        fetch(i, True)

    @pl.when(i + 1 < pl.num_programs(0))
    def _():
        fetch(i + 1, True)

    fetch(i, False)
    o_ref[0] = buf[i % 2].T[:cols, :]


def pieces_transposed(pieces, layer, tp, dp, tp_size, col, cols, prev):
    rows = pieces[0].shape[0]
    n_pieces = len(pieces)
    win = (cols + 127) // 128 * 128
    idx = jnp.stack([tp % 2, tp // 2, dp]).astype(jnp.int32)
    per = tp_size // 2

    def where(i, s):
        return (layer, 0, (s[2] ^ (i // per)) * per + (s[1] ^ (i % per)))

    return pl.pallas_call(
        functools.partial(pieces_t_kernel, col, win, cols, rows, n_pieces),
        grid_spec=pltpu.PrefetchScalarGridSpec(
            num_scalar_prefetch=1,
            grid=(n_pieces // 2,),
            in_specs=[pl.BlockSpec(memory_space=pl.ANY)] * (n_pieces + 1),
            out_specs=pl.BlockSpec((1, cols, 2 * rows), where),
            scratch_shapes=[pltpu.VMEM((2, 2 * rows, win), BF16), pltpu.SemaphoreType.DMA((2, 2))],
        ),
        out_shape=jax.ShapeDtypeStruct(prev.shape, BF16),
        input_output_aliases={n_pieces + 1: 0},
        compiler_params=pltpu.CompilerParams(dimension_semantics=("arbitrary",)),
        cost_estimate=pl.CostEstimate(flops=20 * rows * 8 * win * 128, bytes_accessed=32 * rows * cols, transcendentals=0),
        name="pieces_transposed",
    )(idx, *pieces, prev)


def pieces_rows_kernel(idx_ref, *refs):
    i = pl.program_id(0)
    for k, ref in enumerate(refs[:-1]):
        @pl.when(i == k)
        def _():
            refs[-1][...] = ref[...]


def pieces_rows(pieces, me, cols):
    rows, n_pieces = pieces[0].shape[0], len(pieces)
    return pl.pallas_call(
        pieces_rows_kernel,
        grid_spec=pltpu.PrefetchScalarGridSpec(
            num_scalar_prefetch=1,
            grid=(n_pieces,),
            in_specs=[pl.BlockSpec((rows, cols), lambda i, s: (0, 0))] * n_pieces,
            out_specs=pl.BlockSpec((rows, cols), lambda i, s: (s[0] ^ i, 0)),
        ),
        out_shape=jax.ShapeDtypeStruct((n_pieces * rows, cols), BF16),
        compiler_params=pltpu.CompilerParams(dimension_semantics=("arbitrary",)),
        cost_estimate=pl.CostEstimate(flops=0, bytes_accessed=4 * n_pieces * rows * cols, transcendentals=0),
        name="pieces_rows",
    )(me[None].astype(jnp.int32), *pieces)


def last_rows_kernel(tp_size, dp_size, q_heads, kv_heads, head_dim, len_ref, row_ref, kv_ref, wq_ref, wo_ref, wg_ref, wu_ref, wd_ref, n1_ref, n2_ref, nf_ref, cos_ref, sin_ref, u_ref,
                     g_st, g_rv, a_st, a_rv, s_st, s_rv, f_st, f_rv, q_s, mix_s, rows_s, act_s, send_sem, recv_sem):
    tp, dp = lax.axis_index('tp'), lax.axis_index('dp')
    n_dev = tp_size * dp_size
    shard, ffn_shard = wq_ref.shape[0], wd_ref.shape[0]

    def peer(k):
        return tp ^ (k % tp_size), dp ^ (k // tp_size)

    def slot(k):
        t, d = peer(k)
        return d * tp_size + t

    barrier = pltpu.get_barrier_semaphore()
    for k in range(1, n_dev):
        pl.semaphore_signal(barrier, inc=1, device_id=peer(k), device_id_type=pl.DeviceIdType.MESH)
    pl.semaphore_wait(barrier, n_dev - 1)

    def exchange(step, src, dst):
        copies = [pltpu.make_async_remote_copy(
            src_ref=src(k), dst_ref=dst.at[k], send_sem=send_sem.at[step, k], recv_sem=recv_sem.at[step, k],
            device_id=peer(k), device_id_type=pl.DeviceIdType.MESH) for k in range(1, n_dev)]
        for c in copies:
            c.start()
        for c in copies:
            c.wait()

    def gather(step, value, stage, landed, rows_ref, width):
        for i in range(n_dev):
            stage[i, :, :width] = value[:, i * width:(i + 1) * width]
        exchange(step, lambda k: stage.at[slot(k)], landed)
        rows_ref[0:1, :] = stage[slot(0)]
        for k in range(1, n_dev):
            rows_ref[k:k + 1, :] = landed[k]
        return rows_ref[:, :width].astype(BF16)

    def scatter(step, parts, stage, landed):
        at = 0
        for p in parts:
            for k in range(1, n_dev):
                stage[k, :, at:at + p.shape[1]] = p[k:k + 1, :]
            at += p.shape[1]
        exchange(step, lambda k: stage.at[k], landed)
        out, at = [], 0
        for p in parts:
            total = p[0:1, :]
            for k in range(1, n_dev):
                total = total + landed[k, :, at:at + p.shape[1]]
            out.append(total)
            at += p.shape[1]
        return out

    def norm(hidden, gain_ref):
        return rms_scale(hidden, gain_ref[...]).astype(F32)

    for ref in (g_st, a_st):
        ref[...] = jnp.zeros_like(ref)
    hidden = row_ref[...]
    z = gather(0, norm(hidden, n1_ref), g_st.at[0], g_rv.at[0], rows_s, shard)
    q_row, = scatter(1, [dot32(z, wq_ref[...])], s_st.at[0], s_rv.at[0])
    group = q_heads // kv_heads
    q_s[...] = jnp.zeros_like(q_s)
    for h in range(q_heads):
        piece = q_row[:, h * head_dim:(h + 1) * head_dim]
        at = h // group * 8 + h % group
        q_s[at:at + 1, :] = piece * cos_ref[...] + pltpu.roll(piece, head_dim // 2, 1) * sin_ref[...]
    seq_len = kv_ref.shape[0]
    seen = lax.broadcasted_iota(jnp.int32, (8, seq_len), 1) < len_ref[0]
    for g in range(kv_heads):
        keys = kv_ref[:, g * head_dim:(g + 1) * head_dim]
        values = kv_ref[:, (kv_heads + g) * head_dim:(kv_heads + g + 1) * head_dim]
        scores = lax.dot_general(q_s[g * 8:g * 8 + 8, :].astype(BF16), keys, (((1,), (1,)), ((), ())), preferred_element_type=F32) * head_dim ** -0.5
        scores = jnp.where(seen, scores, -1e30)
        e = jnp.exp(scores - jnp.max(scores, axis=1, keepdims=True))
        probs = (e / jnp.sum(e, axis=1, keepdims=True)).astype(BF16)
        mix = dot32(probs, values).astype(BF16).astype(F32)
        for j in range(group):
            h = g * group + j
            mix_s[:, h * head_dim:(h + 1) * head_dim] = mix[j:j + 1, :]
    z = gather(2, mix_s[...], g_st.at[1], g_rv.at[1], rows_s, shard)
    update, = scatter(3, [dot32(z, wo_ref[...])], s_st.at[1], s_rv.at[1])
    hidden = residual_add(hidden, update.astype(BF16))
    z = gather(4, norm(hidden, n2_ref), g_st.at[2], g_rv.at[2], rows_s, shard)
    gate, up = scatter(5, [dot32(z, wg_ref[...]), dot32(z, wu_ref[...])], f_st, f_rv)
    act = (gate / (1.0 + jnp.exp(-gate)) * up).astype(BF16).astype(F32)
    a = gather(6, act, a_st, a_rv, act_s, ffn_shard)
    update, = scatter(7, [dot32(a, wd_ref[...])], s_st.at[2], s_rv.at[2])
    hidden = residual_add(hidden, update.astype(BF16))
    u_ref[...] = gather(8, norm(hidden, nf_ref), g_st.at[3], g_rv.at[3], rows_s, shard)


def last_rows(mesh, length, row, kv, wq, wo, wg, wu, wd, gains, cos_row, sin_row, q_heads, kv_heads):
    tp_size, dp_size = mesh.shape['tp'], mesh.shape['dp']
    n_dev = tp_size * dp_size
    shard, model_dim = wo.shape
    ffn, ffn_shard = wg.shape[1], wd.shape[0]
    head_dim = cos_row.shape[1]
    pad = lambda n: (n + 127) // 128 * 128
    buf = lambda *lead: pltpu.VMEM(lead[:-1] + (n_dev, 1, lead[-1]), F32)
    vmem = pl.BlockSpec(memory_space=pltpu.VMEM)
    return pl.pallas_call(
        functools.partial(last_rows_kernel, tp_size, dp_size, q_heads, kv_heads, head_dim),
        in_specs=[pl.BlockSpec(memory_space=pltpu.SMEM)] + [vmem] * 12,
        out_specs=vmem,
        out_shape=jax.ShapeDtypeStruct((n_dev, shard), BF16),
        scratch_shapes=[
            buf(4, pad(shard)), buf(4, pad(shard)),
            buf(pad(ffn_shard)), buf(pad(ffn_shard)),
            buf(3, model_dim), buf(3, model_dim),
            buf(2 * ffn), buf(2 * ffn),
            pltpu.VMEM((8 * kv_heads, head_dim), F32),
            pltpu.VMEM((1, q_heads * head_dim), F32),
            pltpu.VMEM((n_dev, pad(shard)), F32),
            pltpu.VMEM((n_dev, pad(ffn_shard)), F32),
            pltpu.SemaphoreType.DMA((9, n_dev)),
            pltpu.SemaphoreType.DMA((9, n_dev)),
        ],
        compiler_params=pltpu.CompilerParams(collective_id=0, has_side_effects=True),
        cost_estimate=pl.CostEstimate(flops=20 * 10**9, bytes_accessed=2 * (wq.size + wo.size + wg.size + wu.size + wd.size), transcendentals=0),
        name="last_rows",
    )(length, row, kv, wq, wo, wg, wu, wd, *gains, cos_row, sin_row)


def split_kernel(starts, widths, *refs):
    o_ref = refs[-1]
    o_ref[...] = jnp.zeros_like(o_ref)
    for ref, start, width in zip(refs[:-1], starts, widths):
        for s in range(o_ref.shape[0]):
            o_ref[s, :, start:start + width] = ref[0, :, s * width:(s + 1) * width]


def split_columns(arrays, n_parts, starts, total):
    rows = arrays[0].shape[1]
    bm = 48
    widths = [a.shape[2] // n_parts for a in arrays]
    last = lambda n: (lambda i: (n - 1, i, 0))
    return pl.pallas_call(
        functools.partial(split_kernel, starts, widths),
        grid=(rows // bm,),
        in_specs=[pl.BlockSpec((1, bm, a.shape[2]), last(a.shape[0])) for a in arrays],
        out_specs=pl.BlockSpec((n_parts, bm, total), lambda i: (0, i, 0)),
        out_shape=jax.ShapeDtypeStruct((n_parts, rows, total), BF16),
        cost_estimate=pl.CostEstimate(flops=20 * rows * total * 128, bytes_accessed=4 * rows * total * n_parts, transcendentals=0),
        name="split_columns",
    )(*arrays)


def attn_kernel(block_rows, head_dim, n_blocks, n_pack, len_ref, q_ref, k_ref, v_ref, o_ref):
    step = pl.program_id(1)
    length = len_ref[0]
    factor = head_dim ** -0.5 * math.log2(math.e)
    trans = (((1,), (1,)), ((), ()))
    for blk in range(n_blocks):
        @pl.when(step == blk)
        def _(blk=blk):
            base = blk * block_rows
            shape = (block_rows, block_rows)
            rows = lax.broadcasted_iota(jnp.int32, shape, 0) + base
            cols = lax.broadcasted_iota(jnp.int32, shape, 1) + base
            diag_ok = cols <= jnp.minimum(rows, length - 1)
            if base:
                past_ok = lax.broadcasted_iota(jnp.int32, (1, base), 1) < length
                past_bias = jnp.where(past_ok, 0.0, -1e30)
            for h in range(n_pack):
                q = q_ref[:, h * head_dim:(h + 1) * head_dim]
                s_diag = lax.dot_general(q, k_ref[base:base + block_rows, :], trans, preferred_element_type=F32)
                s_diag = jnp.where(diag_ok, s_diag, -1e30)
                top = jnp.max(s_diag, axis=1, keepdims=True)
                if base:
                    s_past = lax.dot_general(q, k_ref[:base, :], trans, preferred_element_type=F32) + past_bias
                    top = jnp.maximum(top, jnp.max(s_past, axis=1, keepdims=True))
                shift = top * factor
                e_diag = jnp.exp2(s_diag * factor - shift)
                total = jnp.sum(e_diag, axis=1, keepdims=True)
                if base:
                    e_past = jnp.exp2(s_past * factor - shift)
                    total = total + jnp.sum(e_past, axis=1, keepdims=True)
                inv = 1.0 / total
                mix = dot32((e_diag * inv).astype(BF16), v_ref[base:base + block_rows, :])
                if base:
                    mix = mix + dot32((e_past * inv).astype(BF16), v_ref[:base, :])
                o_ref[:, h * head_dim:(h + 1) * head_dim] = mix.astype(BF16)


def attention(qkv, length, q_heads, kv_heads, head_dim):
    seq_len = qkv.shape[0]
    block_rows = 256
    n_blocks = seq_len // block_rows
    n_pack = 2
    group = q_heads // kv_heads // n_pack
    kern = functools.partial(attn_kernel, block_rows, head_dim, n_blocks, n_pack)
    return pl.pallas_call(
        kern,
        grid=(q_heads // n_pack, n_blocks),
        in_specs=[
            pl.BlockSpec(memory_space=pltpu.SMEM),
            pl.BlockSpec((block_rows, n_pack * head_dim), lambda h, i: (i, h)),
            pl.BlockSpec((seq_len, head_dim), lambda h, i: (0, q_heads + h // group)),
            pl.BlockSpec((seq_len, head_dim), lambda h, i: (0, q_heads + kv_heads + h // group)),
        ],
        out_specs=pl.BlockSpec((block_rows, n_pack * head_dim), lambda h, i: (i, h)),
        out_shape=jax.ShapeDtypeStruct((seq_len, q_heads * head_dim), BF16),
        compiler_params=pltpu.CompilerParams(dimension_semantics=("arbitrary", "arbitrary")),
        cost_estimate=pl.CostEstimate(flops=2 * seq_len * seq_len * q_heads * head_dim * 2, bytes_accessed=4 * seq_len * q_heads * head_dim, transcendentals=seq_len * seq_len * q_heads // 2),
        name="causal_attention",
    )(length, qkv, qkv, qkv)


def solution(mesh):
    tp_size = mesh.shape['tp']
    dp_size = mesh.shape['dp']
    both_axes = ('dp', 'tp')
    both_names = ('tp', 'dp')
    direct_moves, relay_first, relay_second, relay_ends = [], [], [], []
    for t in range(tp_size):
        for d in range(dp_size):
            to_t, to_d = divmod(d * tp_size + t, dp_size)
            if t ^ to_t == tp_size - 1:
                mid = (to_t & 2) | (t & 1)
                relay_first.append((t * dp_size + d, mid * dp_size + d))
                relay_second.append((mid * dp_size + d, to_t * dp_size + to_d))
                relay_ends.append((to_t, to_d))
            else:
                direct_moves.append((t * dp_size + d, to_t * dp_size + to_d))
    swap_cores = [(0, 1), (1, 0)]

    def xor_moves(bit):
        return [(i, i ^ bit) for i in range(tp_size)]

    def gather_all(rows):
        return lax.all_gather(rows, both_axes, axis=0, tiled=True)

    def whole_program(x, lengths, targets, norm1, norm2, norm_f, w_q, w_k, w_v, w_o, w_gate, w_up, w_down, w_lm):
        tp = lax.axis_index('tp')
        dp = lax.axis_index('dp')
        me = dp * tp_size + tp
        q_heads, head_dim = w_q.shape[2], w_q.shape[3]
        kv_heads = w_k.shape[2]
        replicas = tp_size // kv_heads
        n_seq, seq_len, model_dim = x.shape
        loc_heads = q_heads // tp_size
        q_width, kv_width, loc_q = q_heads * head_dim, kv_heads * head_dim, loc_heads * head_dim
        shard = w_q.shape[1]
        ffn = w_gate.shape[2]
        ffn_loc = ffn // tp_size
        my_kv = tp // replicas
        cos_tab, sin_tab = rope_tables(jnp.arange(seq_len), head_dim)
        cos_full = jnp.concatenate([cos_tab, cos_tab], axis=1)
        sin_full = jnp.concatenate([-sin_tab, sin_tab], axis=1)
        mine = tp[None].astype(jnp.int32)
        first = jnp.zeros((1,), jnp.int32)

        flat = lambda w: w.reshape(shard, -1)
        n_layers = w_q.shape[0]
        attn_rows = jnp.concatenate([flat(w_q[0]), flat(w_k[0]), flat(w_v[0]), w_o[0], flat(w_k[1]), flat(w_v[1])], axis=1)
        attn_full = gather_all(attn_rows)
        wg0 = gather_all(w_gate[0])
        wu0 = gather_all(w_up[0])
        cut = model_dim * 2 // 3
        wd0a = gather_all(w_down[0][:, :cut])
        wd0b = gather_all(w_down[0][:, cut:])
        qkv_width = q_width + 2 * kv_width
        kv1_at = qkv_width + q_width
        wo0 = attn_full[:, qkv_width:kv1_at]

        my_head = lambda at: lax.dynamic_slice_in_dim(attn_full, at + my_kv * head_dim, head_dim, 1)
        wk0, wv0 = my_head(q_width), my_head(q_width + kv_width)
        wk1, wv1 = my_head(kv1_at), my_head(kv1_at + kv_width)
        qkv = norm_proj_rope(x, mine, 1, norm1[0], attn_full, 0, qkv_width, q_heads + kv_heads, cos_full, sin_full)
        length = lax.dynamic_index_in_dim(lengths, tp, 0)
        mix = attention(qkv, length, q_heads, kv_heads, head_dim)
        hidden, z = out_proj_norm(x, mine, mix, wo0, norm2[0])
        gate = dot32(z, wg0)
        wkv0 = jnp.concatenate([wk0, wv0], axis=1)
        kv_mine = norm_proj_rope(x, first, n_seq, norm1[0], wkv0, 0, 2 * head_dim, 1, cos_full, sin_full)
        kv_mine = kv_mine.reshape(n_seq, seq_len, 2 * head_dim)
        act = (jax.nn.silu(gate) * dot32(z, wu0)).astype(BF16)
        gate_t = block_transposed(wg0, 0, n_layers, tp * ffn_loc, ffn_loc, None)
        hidden_a = residual_add(hidden[:, :cut], dot32(act, wd0a).astype(BF16))
        up_t = block_transposed(wu0, 0, n_layers, tp * ffn_loc, ffn_loc, None)

        pad = lambda n: (n + 127) // 128 * 128
        starts = [0, pad(loc_q), pad(loc_q) + pad(ffn_loc)]
        total = starts[2] + pad(ffn_loc)
        by_target = split_columns([flat(w_q[1])[None], w_gate, w_up], tp_size, starts, total)
        wo_rows, wd_rows = w_o[1], w_down[1]
        pieces = []
        for bit in range(tp_size):
            piece = lax.dynamic_index_in_dim(by_target, tp ^ bit, 0, keepdims=False)
            if bit:
                piece = lax.ppermute(piece, 'tp', xor_moves(bit))
            pieces.append(piece)

        def to_rows(local_rows):
            moved = lax.ppermute(local_rows, both_names, direct_moves)
            relay = lax.ppermute(local_rows, both_names, relay_first)
            return moved, relay

        wo1, wo_relay = to_rows(wo_rows)
        wd1, wd_relay = to_rows(wd_rows)
        hidden_b = residual_add(hidden[:, cut:], dot32(act, wd0b).astype(BF16))
        hidden = jnp.concatenate([hidden_a, hidden_b], axis=1)

        kv1 = norm_proj_rope(hidden[None], first, 1, norm1[1], attn_full, kv1_at // (2 * kv_width), 2 * kv_width, kv_heads, cos_full, sin_full)
        k1 = lambda i: lax.dynamic_slice_in_dim(kv1, i * head_dim, head_dim, 1)
        v1 = lambda i: lax.dynamic_slice_in_dim(kv1, kv_width + i * head_dim, head_dim, 1)
        k_cache1 = jnp.zeros((n_seq, seq_len, head_dim), BF16)
        v_cache1 = jnp.zeros((n_seq, seq_len, head_dim), BF16)
        for bit in range(tp_size):
            head = (tp ^ bit) // replicas
            piece = jnp.stack([k1(head), v1(head)])
            if bit:
                piece = lax.ppermute(piece, 'tp', xor_moves(bit))
            k_cache1 = lax.dynamic_update_slice(k_cache1, piece[:1], (tp ^ bit, 0, 0))
            v_cache1 = lax.dynamic_update_slice(v_cache1, piece[1:], (tp ^ bit, 0, 0))

        row = lax.dynamic_slice_in_dim(hidden, length[0] - 1, 1, 0)
        cos_r, sin_r = rope_tables(length - 1, head_dim)
        gains = [g.astype(F32)[None] for g in (norm1[1], norm2[1], norm_f)]
        u = last_rows(mesh, length, row, kv1, flat(w_q[1]), w_o[1], w_gate[1], w_up[1], w_down[1], gains,
                      jnp.concatenate([cos_r, cos_r], axis=1), jnp.concatenate([-sin_r, sin_r], axis=1), q_heads, kv_heads)

        part = dot32(u, w_lm)
        part = part[:n_seq] + lax.ppermute(part[n_seq:], 'dp', swap_cores)
        logits = part[:1]
        for bit in range(1, tp_size):
            logits = logits + lax.ppermute(part[bit:bit + 1], 'tp', xor_moves(bit))
        top = jnp.max(logits, axis=1, keepdims=True)
        lse = top + jnp.log(jnp.sum(jnp.exp(logits - top), axis=1, keepdims=True))
        target = lax.dynamic_index_in_dim(targets, tp, 0, keepdims=False)
        hit = jnp.arange(logits.shape[1])[None, :] == target
        logprob = jnp.sum(jnp.where(hit, logits, 0.0), axis=1) - lse[:, 0]
        logprob = lax.all_gather(logprob, 'tp', axis=0, tiled=True)

        relayed = functools.reduce(jnp.logical_or, [jnp.logical_and(tp == t, dp == d) for t, d in relay_ends])
        wo1 = jnp.where(relayed, lax.ppermute(wo_relay, both_names, relay_second), wo1)
        wd1 = jnp.where(relayed, lax.ppermute(wd_relay, both_names, relay_second), wd1)
        pieces = pieces + [lax.ppermute(p, 'dp', swap_cores) for p in pieces]
        wo1b = lax.ppermute(wo1, 'dp', swap_cores)
        wd1b = lax.ppermute(wd1, 'dp', swap_cores)
        heads = lambda w: w.reshape(model_dim, -1, head_dim)

        def pair(a, b):
            out = jnp.zeros((2,) + a.shape, BF16)
            return lax.dynamic_update_slice(lax.dynamic_update_slice(out, a[None], (dp, 0, 0)), b[None], (1 - dp, 0, 0)).reshape(2 * a.shape[0], a.shape[1])

        wq1 = pieces_rows(pieces, me, loc_q)
        q_out = jnp.stack([heads(lax.dynamic_slice_in_dim(attn_full, tp * loc_q, loc_q, 1)), heads(wq1)])
        k_out = jnp.stack([heads(wk0), heads(wk1)])
        v_out = jnp.stack([heads(wv0), heads(wv1)])
        o_out = jnp.stack([lax.dynamic_slice_in_dim(wo0, tp * loc_q, loc_q, 0), pair(wo1, wo1b)])
        gate_t = pieces_transposed(pieces, 1, tp, dp, tp_size, starts[1], ffn_loc, gate_t)
        up_t = pieces_transposed(pieces, 1, tp, dp, tp_size, starts[2], ffn_loc, up_t)
        gate_out = jnp.swapaxes(gate_t, 1, 2)
        up_out = jnp.swapaxes(up_t, 1, 2)
        rows_of = lambda w: lax.dynamic_slice_in_dim(w, tp * ffn_loc, ffn_loc, 0)
        down_out = jnp.stack([jnp.concatenate([rows_of(wd0a), rows_of(wd0b)], axis=1), pair(wd1, wd1b)])
        k_cache = jnp.stack([kv_mine[:, :, :head_dim], k_cache1])[:, :, None]
        v_cache = jnp.stack([kv_mine[:, :, head_dim:], v_cache1])[:, :, None]
        return (q_out, k_out, v_out, o_out, gate_out, up_out, down_out, k_cache, v_cache, logprob)

    row_split = P(None, ('dp', 'tp'), None)
    head_rows = P(None, ('dp', 'tp'), None, None)
    head_cols = P(None, None, 'tp', None)
    col_split = P(None, None, 'tp')
    row_tp = P(None, 'tp', None)
    cache_spec = P(None, 'dp', 'tp', None, None)
    in_specs = (P('dp', None, None), P('dp'), P('dp'), P(), P(), P(), head_rows, head_rows, head_rows, row_split, row_split, row_split, row_split, P(('dp', 'tp'), None))
    out_specs = (head_cols, head_cols, head_cols, row_tp, col_split, col_split, row_tp, cache_spec, cache_spec, P('dp'))
    return jax.shard_map(whole_program, mesh=mesh, in_specs=in_specs, out_specs=out_specs, check_vma=False)
```
